32 devices in a mesh: gx: 2 (over y), gy: 4 (over x, core), gz: 4 (over z).
Axes of the slice: x: 2, y: 2, z: 4, core: 2. Of those that a mesh axis runs over, the one named last changes fastest.
Arguments:
- occupancy: int32 [32, 256, 512], P('gx', 'gy', 'gz'), may hold values 0 or 1
- site_field: float32 [32, 256, 512], P('gx', 'gy', 'gz'), may hold values from -6 to 6
- attempt_rate: float32 [32, 256, 512], P('gx', 'gy', 'gz'), may hold values from 0.2 to 5
- uniforms: float32 [8, 32, 256, 256], P(None, 'gx', 'gy', 'gz'), may hold values from 0.001 to 1
Outputs:
- final_spins: float32 [32, 256, 512], P('gx', 'gy', 'gz')
- history: float32 [2, 8], replicated
The draws below stay inside these ranges and needn't reach their ends.
All inputs are finite; a program needn't handle non-finite values. No bound on the sum of `occupancy` on one device may be relied on, other than what follows from the above.
Results may differ from the reference program's by a relative error of at most 0.0002.
Values sent between devices are 32-bit elements; how exact they have to be, the bound alone decides.
A program may use at most 128 MiB of HBM per device.

```python
import math
import jax
import jax.numpy as jnp
from jax import lax

SECTIONS = 8
NX = 32
NY = 256
NZ = 512


def place_ends(values, rng, least, largest):
    longest = values.shape.index(max(values.shape))
    spots = []
    for shift in (0, 1):
        where = [jax.random.randint(jax.random.fold_in(rng, axis), (), 0, length) for axis, length in enumerate(values.shape)]
        where[longest] = (where[longest] + shift) % values.shape[longest]
        spots.append(tuple(where))
    return values.at[spots[0]].set(least).at[spots[1]].set(largest)


def level_of(key, shape, cuts, smallest, largest):
    loudness, own = 1.0, jax.random.fold_in(key, 6)
    for dim, blocks in cuts:
        heights = jnp.exp(jax.random.uniform(jax.random.fold_in(own, dim), (blocks,), jnp.float32, smallest / len(cuts), largest / len(cuts)))
        loudness = loudness * jnp.repeat(heights, shape[dim] // blocks).reshape([-1 if axis == dim else 1 for axis in range(len(shape))])
    return loudness


def bell_draw(rng, extent, width, most, shards=(), held_as=jnp.bfloat16):
    array = jax.random.normal(rng, extent, jnp.float32) * width
    if len(shards) > 0:
        array = level_of(rng, extent, shards, -0.22, 0.18) * array
    return jnp.clip(array, min=-most, max=most).astype(held_as)


def setup_inputs(seed: int = 0) -> dict:
    key_of = jax.random.split(jax.random.key(seed), 5)
    occupancy = place_ends((jax.random.randint(key_of[0], (NX, NY, NZ), 0, 2) < 1).astype(jnp.int32), jax.random.fold_in(key_of[0], 1), 0, 1)
    site_field = bell_draw(key_of[1], (NX, NY, NZ), 1.0, 6.0, ((0, 2), (1, 4), (2, 4)), jnp.float32)
    attempt_rate = jnp.clip(jnp.exp(math.log(5.0) - 3.218876 * jax.random.uniform(key_of[2], (NX, NY, NZ), jnp.float32) ** level_of(key_of[2], (NX, NY, NZ), ((0, 2), (1, 4), (2, 4)), -0.2, 0.2)), 0.2, 5.0)
    uniforms = jnp.clip(0.001 + 0.999 * jax.random.uniform(key_of[3], (SECTIONS, NX, NY, NZ // 2), jnp.float32) ** level_of(key_of[3], (SECTIONS, NX, NY, NZ // 2), ((1, 2), (2, 4), (3, 4)), -0.2, 0.2), 0.001, 1.0)
    return dict(occupancy=occupancy, site_field=site_field, attempt_rate=attempt_rate, uniforms=uniforms)


coupling = 0.5
softness = 0.5


def neighbours(spin):
    total = jnp.roll(spin, 1, 0) + jnp.roll(spin, -1, 0)
    total = total + jnp.roll(spin, 1, 1) + jnp.roll(spin, -1, 1)
    return total + jnp.roll(spin, 1, 2) + jnp.roll(spin, -1, 2)


def parity_mask(shape, phase):
    xpos = lax.broadcasted_iota(jnp.int32, shape, 0)
    ypos = lax.broadcasted_iota(jnp.int32, shape, 1)
    zpos = lax.broadcasted_iota(jnp.int32, shape, 2)
    return (((xpos + ypos + zpos) % 2) == phase).astype(jnp.float32)


def unpack_draws(packed, phase):
    shape = packed.shape
    xpos = lax.broadcasted_iota(jnp.int32, shape, 0)
    ypos = lax.broadcasted_iota(jnp.int32, shape, 1)
    select = (xpos + ypos + phase) % 2
    first = jnp.where(select == 0, packed, jnp.float32(1.0))
    second = jnp.where(select == 1, packed, jnp.float32(1.0))
    return jnp.stack([first, second], -1).reshape(shape[0], shape[1], 2 * shape[2])


def reference(occupancy, site_field, attempt_rate, uniforms):
    spin = 2.0 * occupancy.astype(jnp.float32) - 1.0
    sites_total = spin.size
    half_sites = sites_total / 2.0
    clock = jnp.float32(0.0)
    energies = []
    times = []
    for section_index in range(SECTIONS):
        phase = section_index % 2
        mask = parity_mask(spin.shape, phase)
        beside_all = neighbours(spin)
        delta = 2.0 * spin * (site_field - coupling * beside_all)
        rate_log = jnp.log(attempt_rate) - jax.nn.softplus(delta)
        total_rate = jnp.sum(mask * jnp.exp(rate_log))
        log_dt = jnp.log(jnp.float32(half_sites)) - jnp.log(total_rate)
        draws_full = unpack_draws(uniforms[section_index], phase)
        accept = jax.nn.sigmoid((rate_log + log_dt - jnp.log(draws_full)) / softness)
        spin = spin - 2.0 * accept * spin * mask
        energy = (coupling * jnp.sum(mask * spin * beside_all) - jnp.sum(site_field * spin)) / sites_total
        clock = clock + half_sites / total_rate
        energies.append(energy)
        times.append(clock)
    history = jnp.stack([jnp.stack(energies), jnp.stack(times)]).astype(jnp.float32)
    return spin, history
```

```python
import functools
import itertools

import jax
import jax.numpy as jnp
from jax import lax
from jax.experimental import pallas as pl
from jax.experimental.pallas import tpu as pltpu
from jax.sharding import PartitionSpec as P

SECTIONS = 8
AXES = ("gx", "gy", "gz")
MESH = pl.DeviceIdType.MESH
PAD = 8


def kernel(sizes, occ, fld, att, uni, out, hist, spin, field, rate0, inv, draw, ratio, local, ghost, hsend, hrecv,
           rsend, rrecv, hs, hr, rs, rr):
    gx, gy, gz = sizes
    count = gx * gy * gz
    planes, rows, lanes = ratio.shape
    half = lanes // 2
    tiles = rows // 8
    body = pl.ds(PAD, rows)
    xdirs = 1 if gx == 2 else 2
    ybase, zbase = tiles * xdirs, tiles * xdirs + 2
    half_sites = float(planes * rows * lanes * count)
    pos = [lax.axis_index(axis) for axis in AXES]
    me = (pos[0] * gy + pos[1]) * gz + pos[2]
    moved = [[lax.rem(pos[a] + d, sizes[a]) for d in range(sizes[a])] for a in range(3)]

    def device(dx, dy, dz):
        return (moved[0][dx % gx], moved[1][dy % gy], moved[2][dz % gz])

    others = [o for o in itertools.product(range(gx), range(gy), range(gz)) if o != (0, 0, 0)]
    others.sort(key=lambda o: -(min(o[0], gx - o[0]) + min(o[1], gy - o[1]) + 2 * min(o[2], gz - o[2])))

    barrier = pltpu.get_barrier_semaphore()
    for o in others:
        pl.semaphore_signal(barrier, inc=1, device_id=device(*o), device_id_type=MESH)

    lane = lax.broadcasted_iota(jnp.int32, (rows, lanes), 1)
    row = lax.broadcasted_iota(jnp.int32, (rows, lanes), 0)
    low = lane < half
    place = lax.rem(lane, half)
    last = place == half - 1
    even = (row & 1) == 0
    odd = (row & 1) == 1
    lane8 = lax.broadcasted_iota(jnp.int32, (8, lanes), 1)
    row8 = lax.broadcasted_iota(jnp.int32, (8, lanes), 0)

    def kind(parity):
        return even if parity % 2 == 0 else odd

    def turn(x, shift):
        return pltpu.roll(x, shift % lanes, 1)

    zrow = lax.broadcasted_iota(jnp.int32, (lanes, lanes), 0)
    zcol = lax.broadcasted_iota(jnp.int32, (lanes, lanes), 1)
    split = (zrow == 2 * lax.rem(zcol, half) + zcol // half).astype(jnp.float32)
    join = (zcol == 2 * lax.rem(zrow, half) + zrow // half).astype(jnp.float32)

    def exact(a, b):
        return jnp.dot(a, b, precision=lax.Precision.HIGHEST, preferred_element_type=jnp.float32)

    def packed(ref, xi):
        first = exact(ref[xi].astype(jnp.float32), split)
        second = exact(ref[xi + planes].astype(jnp.float32), split)
        evens = jnp.where(low, first, turn(second, half))
        odds = jnp.where(low, turn(first, half), second)
        flip = ((row + xi) & 1) == 1
        return jnp.where(flip, odds, evens), jnp.where(flip, evens, odds)

    def prepare(xi, sums):
        s = packed(occ, xi)
        f = packed(fld, xi)
        a = packed(att, xi)
        for p in range(2):
            spin[p, xi + 1, body, :] = 2.0 * s[p] - 1.0
            field[p, xi] = f[p]
            rate0[p, xi] = a[p]
            inv[p, xi] = 1.0 / a[p]
        return sums + fold(f[1] * (2.0 * s[1] - 1.0))

    def fold(x):
        return jnp.sum(x.reshape(tiles, 8, lanes), axis=0)

    zero = jnp.zeros((8, lanes), jnp.float32)
    field_sum = lax.fori_loop(0, planes, prepare, zero)

    def set_draws(k, p):
        for xi in range(planes):
            both = jnp.concatenate([uni[k, xi], uni[k, xi + planes]], axis=1)
            draw[xi] = both * inv[p, xi]

    def halo_copies(slot):
        src = hsend.at[slot]
        up_x, down_x = device(1, 0, 0), device(-1, 0, 0)
        dst = hrecv.at[slot]
        moves = []
        if xdirs == 1:
            moves.append((pl.ds(0, tiles), pl.ds(0, tiles), up_x))
        else:
            moves.append((pl.ds(0, tiles), pl.ds(0, tiles), down_x))
            moves.append((pl.ds(0, tiles), pl.ds(tiles, tiles), up_x))
        moves.append((pl.ds(tiles, 1), pl.ds(ybase, 1), device(0, -1, 0)))
        moves.append((pl.ds(tiles + 1, 1), pl.ds(ybase + 1, 1), device(0, 1, 0)))
        moves.append((pl.ds(tiles + 2, 1), pl.ds(zbase, 1), device(0, 0, 1)))
        moves.append((pl.ds(tiles + 2, 1), pl.ds(zbase + 1, 1), device(0, 0, -1)))
        for a, b, target in moves:
            pltpu.make_async_remote_copy(src.at[a], dst.at[b], hs.at[slot], hr.at[slot], device_id=target, device_id_type=MESH).start()

    def send_halo(slot, plane, user):
        hsend[slot, pl.ds(0, tiles)] = jnp.where(low, plane(0), plane(planes - 1)).reshape(tiles, 8, lanes)
        tail = jnp.zeros((rows, lanes), jnp.float32)
        for xi in range(planes):
            full = plane(xi)
            hsend[slot, tiles, pl.ds(xi, 1), :] = full[0:1]
            hsend[slot, tiles + 1, pl.ds(xi, 1), :] = full[rows - 1:rows]
            ends = jnp.where(kind(xi + user), full, turn(full, -1))
            tail = tail + jnp.where(place == half - 1 - xi, turn(ends, -xi), 0.0)
        z = tail[0:8]
        for t in range(1, tiles):
            z = z + turn(tail[8 * t:8 * t + 8], -planes * t)
        hsend[slot, tiles + 2] = z
        halo_copies(slot)

    def wait_halo(slot):
        whole = hrecv.at[slot]
        pltpu.make_async_copy(whole, whole, hr.at[slot]).wait()
        pltpu.make_async_copy(whole, whole, hs.at[slot]).wait()

    def received(slot, user):
        xs = hrecv[slot, pl.ds(0, tiles)].reshape(rows, lanes)
        if xdirs == 2:
            xs = jnp.where(low, xs, hrecv[slot, pl.ds(tiles, tiles)].reshape(rows, lanes))
        ys = (hrecv[slot, ybase], hrecv[slot, ybase + 1])
        down = ((lane8 + 1 + row8 + user) & 1) == 0
        return xs, ys, jnp.where(down, hrecv[slot, zbase], hrecv[slot, zbase + 1])

    def store_ghosts(p, xs, ys, zs):
        ghost[p, pl.ds(0, tiles)] = xs.reshape(tiles, 8, lanes)
        ghost[p, tiles], ghost[p, tiles + 1] = ys
        ghost[p, tiles + 2] = zs

    def load_ghosts(p):
        return ghost[p, pl.ds(0, tiles)].reshape(rows, lanes), (ghost[p, tiles], ghost[p, tiles + 1]), ghost[p, tiles + 2]

    def place_ghosts(p):
        xs, (above, below), _ = load_ghosts(p)
        spin[p, 0, body, :] = turn(jnp.where(low, spin[p, planes, body, :], xs), half)
        spin[p, planes + 1, body, :] = turn(jnp.where(low, xs, spin[p, 1, body, :]), half)
        for xi in range(planes):
            spin[p, xi + 1, pl.ds(PAD - 1, 1), :] = below[xi:xi + 1]
            spin[p, xi + 1, pl.ds(PAD + rows, 1), :] = above[xi:xi + 1]

    def rates(q):
        p = 1 - q
        zs = ghost[p, tiles + 2]
        ztile = jnp.concatenate([turn(zs, planes * t + half) for t in range(tiles)], axis=0)
        total = zero
        for xi in range(planes):
            mid = spin[p, xi + 1, body, :]
            edge = turn(ztile, xi)
            before = turn(jnp.where(last, edge, mid), 1)
            after = jnp.where(last, edge, turn(mid, -1))
            beside = spin[p, xi, body, :] + spin[p, xi + 2, body, :]
            beside = beside + spin[p, xi + 1, pl.ds(PAD - 1, rows), :] + spin[p, xi + 1, pl.ds(PAD + 1, rows), :]
            beside = beside + mid + jnp.where(kind(xi + q), before, after)
            h = field[q, xi] - 0.5 * beside
            grown = 1.0 + jnp.exp(2.0 * spin[q, xi + 1, body, :] * h)
            r = draw[xi] * grown
            ratio[xi] = r * r
            local[xi] = h
            total = total + fold(rate0[q, xi] / grown)
        return total

    def send_rates(slot, rate, energy):
        both = jnp.where(lane8 < half, rate + turn(rate, half), energy + turn(energy, half))
        message = jnp.sum(both, axis=0, keepdims=True)
        rsend[slot] = message
        rrecv[slot, me] = message
        for o in others:
            pltpu.make_async_remote_copy(rsend.at[slot], rrecv.at[slot, me], rs.at[slot], rr.at[slot],
                                         device_id=device(*o), device_id_type=MESH).start()

    def wait_rates(slot):
        most = rrecv.at[slot, pl.ds(0, count - 1)]
        pltpu.make_async_copy(most, most, rr.at[slot]).wait()
        pltpu.make_async_copy(most, most, rs.at[slot]).wait()
        total = jnp.sum(rrecv[slot], axis=0)
        first = lax.broadcasted_iota(jnp.int32, (1, lanes), 1) < half
        rate = jnp.sum(jnp.where(first, total, 0.0), axis=1, keepdims=True)
        energy = jnp.sum(jnp.where(first, 0.0, total), axis=1, keepdims=True)
        return rate, energy

    def section(k, p, carry, final):
        fields, energy, clock, table = carry
        q = 1 - p
        if not final:
            set_draws(k + 1, q)
        rate, old = wait_rates(p)
        table = jnp.where((row8 == 0) & (lane8 == k - 1), old / (2.0 * half_sites), table)
        clock = clock + half_sites / rate
        table = jnp.where((row8 == 1) & (lane8 == k), clock, table)
        scaled = rate * (1.0 / half_sites)
        c = scaled * scaled

        def after(s, x):
            xc = x * c
            return s * ((xc - 1.0) / (xc + 1.0))

        energy, own = -fields, zero
        for xi in range(planes):
            s = after(spin[p, xi + 1, body, :], ratio[xi])
            spin[p, xi + 1, body, :] = s
            energy = energy - fold(s * local[xi])
            own = own + fold(s * field[p, xi])
        wait_halo(p)
        if not final:
            gx_, gy_, gz_ = load_ghosts(p)
            nx_, ny_, nz_ = received(p, q)
            store_ghosts(p, after(gx_, nx_), (after(gy_[0], ny_[0]), after(gy_[1], ny_[1])), after(gz_, nz_))
            place_ghosts(p)
            send_rates(q, rates(q), energy)
            send_halo(q, lambda xi: ratio[xi], p)
        return own, energy, clock, table

    pl.semaphore_wait(barrier, count - 1)
    for p in range(2):
        send_halo(2 + p, lambda xi: spin[p, xi + 1, body, :], 1 - p)
    set_draws(0, 0)
    for p in (1, 0):
        wait_halo(2 + p)
        store_ghosts(p, *received(2 + p, 1 - p))
    place_ghosts(1)
    send_rates(0, rates(0), zero)
    send_halo(0, lambda xi: ratio[xi], 1)

    def pair(m, carry):
        carry = section(2 * m, 0, carry, False)
        return section(2 * m + 1, 1, carry, False)

    carry = (field_sum, zero, jnp.zeros((1, 1), jnp.float32), zero)
    carry = lax.fori_loop(0, SECTIONS // 2 - 1, pair, carry)
    carry = section(SECTIONS - 2, 0, carry, False)
    _, energy, _, table = section(SECTIONS - 1, 1, carry, True)
    send_rates(0, zero, energy)

    def finish(xi, none):
        flip = ((row + xi) & 1) == 1
        e, o = spin[0, xi + 1, body, :], spin[1, xi + 1, body, :]
        evens, odds = jnp.where(flip, o, e), jnp.where(flip, e, o)
        out[xi] = exact(jnp.where(low, evens, turn(odds, half)), join)
        out[xi + planes] = exact(jnp.where(low, turn(evens, half), odds), join)
        return none

    lax.fori_loop(0, planes, finish, 0)
    _, old = wait_rates(0)
    table = jnp.where((row8 == 0) & (lane8 == SECTIONS - 1), old / (2.0 * half_sites), table)
    hist[...] = table[0:2, 0:SECTIONS]


def solution(mesh):
    sizes = tuple(mesh.shape[axis] for axis in AXES)

    def step(occupancy, site_field, attempt_rate, uniforms):
        nx, ny, nz = occupancy.shape
        planes = nx // 2
        tiles = ny // 8
        assert nx % 4 == 0 and ny % 8 == 0 and nz % 128 == 0 and planes * tiles <= nz // 2
        xdirs = 1 if sizes[0] == 2 else 2
        count = sizes[0] * sizes[1] * sizes[2]
        vmem = functools.partial(pl.BlockSpec, memory_space=pltpu.VMEM)
        f32 = jnp.float32
        return pl.pallas_call(
            functools.partial(kernel, sizes),
            out_shape=(jax.ShapeDtypeStruct((nx, ny, nz), f32), jax.ShapeDtypeStruct((2, SECTIONS), f32)),
            in_specs=[vmem()] * 4,
            out_specs=(vmem(), vmem()),
            scratch_shapes=[
                pltpu.VMEM((2, planes + 2, ny + 2 * PAD, nz), f32),
                pltpu.VMEM((2, planes, ny, nz), f32),
                pltpu.VMEM((2, planes, ny, nz), f32),
                pltpu.VMEM((2, planes, ny, nz), f32),
                pltpu.VMEM((planes, ny, nz), f32),
                pltpu.VMEM((planes, ny, nz), f32),
                pltpu.VMEM((planes, ny, nz), f32),
                pltpu.VMEM((2, tiles + 3, 8, nz), f32),
                pltpu.VMEM((4, tiles + 3, 8, nz), f32),
                pltpu.VMEM((4, tiles * xdirs + 4, 8, nz), f32),
                pltpu.VMEM((2, 1, nz), f32),
                pltpu.VMEM((2, count, 1, nz), f32),
                pltpu.SemaphoreType.DMA((4,)),
                pltpu.SemaphoreType.DMA((4,)),
                pltpu.SemaphoreType.DMA((2,)),
                pltpu.SemaphoreType.DMA((2,)),
            ],
            compiler_params=pltpu.CompilerParams(collective_id=0, has_side_effects=True),
        )(occupancy, site_field, attempt_rate, uniforms)

    in_specs = (P("gx", "gy", "gz"), P("gx", "gy", "gz"), P("gx", "gy", "gz"), P(None, "gx", "gy", "gz"))
    return jax.shard_map(step, mesh=mesh, in_specs=in_specs, out_specs=(P("gx", "gy", "gz"), P()), check_vma=False)
```

```python
import functools
import itertools

import jax
import jax.numpy as jnp
from jax import lax
from jax.experimental import pallas as pl
from jax.experimental.pallas import tpu as pltpu
from jax.sharding import PartitionSpec as P

SECTIONS = 8
AXES = ("gx", "gy", "gz")
MESH = pl.DeviceIdType.MESH
PAD = 8


def kernel(sizes, occ_hbm, fld_hbm, att_hbm, uni_hbm, out, hist, occ, fld, att, uni, loaded, spin, field, rate0, inv, draw, ratio, local, ghost, hsend, hrecv,
           rsend, rrecv, hs, hr, rs, rr):
    gx, gy, gz = sizes
    count = gx * gy * gz
    planes, rows, lanes = ratio.shape
    half = lanes // 2
    tiles = rows // 8
    body = pl.ds(PAD, rows)
    xdirs = 1 if gx == 2 else 2
    ybase, zbase = tiles * xdirs, tiles * xdirs + 2
    loads = [pltpu.make_async_copy(a, b, loaded.at[i]) for i, (a, b) in enumerate(((occ_hbm, occ), (fld_hbm, fld), (att_hbm, att), (uni_hbm, uni)))]
    for load in loads:
        load.start()
    half_sites = float(planes * rows * lanes * count)
    pos = [lax.axis_index(axis) for axis in AXES]
    me = (pos[0] * gy + pos[1]) * gz + pos[2]
    moved = [[lax.rem(pos[a] + d, sizes[a]) for d in range(sizes[a])] for a in range(3)]

    def device(dx, dy, dz):
        return (moved[0][dx % gx], moved[1][dy % gy], moved[2][dz % gz])

    others = [o for o in itertools.product(range(gx), range(gy), range(gz)) if o != (0, 0, 0)]
    others.sort(key=lambda o: -(min(o[0], gx - o[0]) + min(o[1], gy - o[1]) + 4 * (o[2] % 2) + 2 * (o[2] > 0)))

    barrier = pltpu.get_barrier_semaphore()
    for o in others:
        pl.semaphore_signal(barrier, inc=1, device_id=device(*o), device_id_type=MESH)

    lane = lax.broadcasted_iota(jnp.int32, (rows, lanes), 1)
    row = lax.broadcasted_iota(jnp.int32, (rows, lanes), 0)
    low = lane < half
    place = lax.rem(lane, half)
    last = place == half - 1
    even = (row & 1) == 0
    odd = (row & 1) == 1
    lane8 = lax.broadcasted_iota(jnp.int32, (8, lanes), 1)
    row8 = lax.broadcasted_iota(jnp.int32, (8, lanes), 0)

    def kind(parity):
        return even if parity % 2 == 0 else odd

    def turn(x, shift):
        return pltpu.roll(x, shift % lanes, 1)

    zrow = lax.broadcasted_iota(jnp.int32, (lanes, lanes), 0)
    zcol = lax.broadcasted_iota(jnp.int32, (lanes, lanes), 1)
    split = (zrow == 2 * lax.rem(zcol, half) + zcol // half).astype(jnp.float32)
    join = (zcol == 2 * lax.rem(zrow, half) + zrow // half).astype(jnp.float32)

    def exact(a, b):
        return jnp.dot(a, b, precision=lax.Precision.HIGHEST, preferred_element_type=jnp.float32)

    split16 = split.astype(jnp.bfloat16)
    split48 = jnp.concatenate([split16] * 3, axis=0)

    def packed(ref, xi, n, whole):
        both = jnp.concatenate([ref[pl.ds(xi, n)].reshape(n * rows, lanes), ref[pl.ds(xi + planes, n)].reshape(n * rows, lanes)], axis=0)
        if whole:
            parts = both.astype(jnp.float32).astype(jnp.bfloat16)
        else:
            high = both.astype(jnp.bfloat16)
            rest = both - high.astype(jnp.float32)
            middle = rest.astype(jnp.bfloat16)
            parts = jnp.concatenate([high, middle, (rest - middle.astype(jnp.float32)).astype(jnp.bfloat16)], axis=1)
        moved = jnp.dot(parts, split16 if whole else split48, preferred_element_type=jnp.float32)
        for i in range(n):
            first, second = moved[i * rows:(i + 1) * rows], moved[(n + i) * rows:(n + i + 1) * rows]
            evens = jnp.where(low, first, turn(second, half))
            odds = jnp.where(low, turn(first, half), second)
            flip = ((row + xi + i) & 1) == 1
            yield xi + i, (jnp.where(flip, odds, evens), jnp.where(flip, evens, odds))

    def prepare_spins(group, none):
        for xi, s in packed(occ, 2 * group, 2, True):
            for p in range(2):
                spin[p, xi + 1, body, :] = 2.0 * s[p] - 1.0
        return none

    def prepare_rest(group, sums):
        for xi, f in packed(fld, 2 * group, 2, False):
            for p in range(2):
                field[p, xi] = f[p]
            sums = sums + fold(f[1] * spin[1, xi + 1, body, :])
        for xi, a in packed(att, 2 * group, 2, False):
            for p in range(2):
                rate0[p, xi] = a[p]
                inv[p, xi] = 1.0 / a[p]
        return sums

    def fold(x):
        return jnp.sum(x.reshape(tiles, 8, lanes), axis=0)

    zero = jnp.zeros((8, lanes), jnp.float32)
    loads[0].wait()
    lax.fori_loop(0, planes // 2, prepare_spins, 0)

    def set_draws(k, p):
        for xi in range(planes):
            both = jnp.concatenate([uni[k, xi], uni[k, xi + planes]], axis=1)
            draw[xi] = both * inv[p, xi]

    def halo_copy(slot, a, b, n, target):
        pltpu.make_async_remote_copy(hsend.at[slot, pl.ds(a, n)], hrecv.at[slot, pl.ds(b, n)], hs.at[slot], hr.at[slot],
                                     device_id=target, device_id_type=MESH).start()

    def send_halo(slot, plane, user):
        tail = jnp.zeros((rows, lanes), jnp.float32)
        for xi in range(planes):
            full = plane(xi)
            ends = jnp.where(kind(xi + user), full, turn(full, -1))
            tail = tail + jnp.where(place == half - 1 - xi, turn(ends, -xi), 0.0)
        z = tail[0:8]
        for t in range(1, tiles):
            z = z + turn(tail[8 * t:8 * t + 8], -planes * t)
        hsend[slot, tiles + 2] = z
        halo_copy(slot, tiles + 2, zbase, 1, device(0, 0, 1))
        halo_copy(slot, tiles + 2, zbase + 1, 1, device(0, 0, -1))
        hsend[slot, pl.ds(0, tiles)] = jnp.where(low, plane(0), plane(planes - 1)).reshape(tiles, 8, lanes)
        if xdirs == 1:
            halo_copy(slot, 0, 0, tiles, device(1, 0, 0))
        else:
            halo_copy(slot, 0, 0, tiles, device(-1, 0, 0))
            halo_copy(slot, 0, tiles, tiles, device(1, 0, 0))
        for xi in range(planes):
            full = plane(xi)
            hsend[slot, tiles, pl.ds(xi, 1), :] = full[0:1]
            hsend[slot, tiles + 1, pl.ds(xi, 1), :] = full[rows - 1:rows]
        halo_copy(slot, tiles, ybase, 1, device(0, -1, 0))
        halo_copy(slot, tiles + 1, ybase + 1, 1, device(0, 1, 0))

    def wait_halo(slot):
        whole = hrecv.at[slot]
        pltpu.make_async_copy(whole, whole, hr.at[slot]).wait()
        pltpu.make_async_copy(whole, whole, hs.at[slot]).wait()

    def received(slot, user):
        xs = hrecv[slot, pl.ds(0, tiles)].reshape(rows, lanes)
        if xdirs == 2:
            xs = jnp.where(low, xs, hrecv[slot, pl.ds(tiles, tiles)].reshape(rows, lanes))
        ys = (hrecv[slot, ybase], hrecv[slot, ybase + 1])
        down = ((lane8 + 1 + row8 + user) & 1) == 0
        return xs, ys, jnp.where(down, hrecv[slot, zbase], hrecv[slot, zbase + 1])

    def store_ghosts(p, xs, ys, zs):
        ghost[p, pl.ds(0, tiles)] = xs.reshape(tiles, 8, lanes)
        ghost[p, tiles], ghost[p, tiles + 1] = ys
        ghost[p, tiles + 2] = zs

    def load_ghosts(p):
        return ghost[p, pl.ds(0, tiles)].reshape(rows, lanes), (ghost[p, tiles], ghost[p, tiles + 1]), ghost[p, tiles + 2]

    def place_ghosts(p):
        xs, (above, below), _ = load_ghosts(p)
        spin[p, 0, body, :] = turn(jnp.where(low, spin[p, planes, body, :], xs), half)
        spin[p, planes + 1, body, :] = turn(jnp.where(low, xs, spin[p, 1, body, :]), half)
        for xi in range(planes):
            spin[p, xi + 1, pl.ds(PAD - 1, 1), :] = below[xi:xi + 1]
            spin[p, xi + 1, pl.ds(PAD + rows, 1), :] = above[xi:xi + 1]

    def rates(q):
        p = 1 - q
        zs = ghost[p, tiles + 2]
        ztile = jnp.concatenate([turn(zs, planes * t + half) for t in range(tiles)], axis=0)
        total = zero
        for xi in range(planes):
            mid = spin[p, xi + 1, body, :]
            edge = turn(ztile, xi)
            before = turn(jnp.where(last, edge, mid), 1)
            after = jnp.where(last, edge, turn(mid, -1))
            beside = spin[p, xi, body, :] + spin[p, xi + 2, body, :]
            beside = beside + spin[p, xi + 1, pl.ds(PAD - 1, rows), :] + spin[p, xi + 1, pl.ds(PAD + 1, rows), :]
            beside = beside + mid + jnp.where(kind(xi + q), before, after)
            h = field[q, xi] - 0.5 * beside
            grown = 1.0 + jnp.exp(2.0 * spin[q, xi + 1, body, :] * h)
            r = draw[xi] * grown
            ratio[xi] = r * r
            local[xi] = h
            total = total + fold(rate0[q, xi] / grown)
        return total

    def send_rates(slot, rate, energy):
        both = jnp.where(lane8 < half, rate + turn(rate, half), energy + turn(energy, half))
        message = jnp.sum(both, axis=0, keepdims=True)
        rsend[slot] = message
        rrecv[slot, me] = message
        for o in others:
            pltpu.make_async_remote_copy(rsend.at[slot], rrecv.at[slot, me], rs.at[slot], rr.at[slot],
                                         device_id=device(*o), device_id_type=MESH).start()

    def wait_rates(slot):
        most = rrecv.at[slot, pl.ds(0, count - 1)]
        pltpu.make_async_copy(most, most, rr.at[slot]).wait()
        pltpu.make_async_copy(most, most, rs.at[slot]).wait()
        total = jnp.sum(rrecv[slot], axis=0)
        first = lax.broadcasted_iota(jnp.int32, (1, lanes), 1) < half
        rate = jnp.sum(jnp.where(first, total, 0.0), axis=1, keepdims=True)
        energy = jnp.sum(jnp.where(first, 0.0, total), axis=1, keepdims=True)
        return rate, energy

    def section(k, p, carry, final):
        fields, energy, clock, table = carry
        q = 1 - p
        if not final:
            set_draws(k + 1, q)
        rate, old = wait_rates(p)
        table = jnp.where((row8 == 0) & (lane8 == k - 1), old / (2.0 * half_sites), table)
        clock = clock + half_sites / rate
        table = jnp.where((row8 == 1) & (lane8 == k), clock, table)
        scaled = rate * (1.0 / half_sites)
        c = scaled * scaled

        def after(s, x):
            xc = x * c
            return s * ((xc - 1.0) / (xc + 1.0))

        energy, own = -fields, zero
        for xi in range(planes):
            s = after(spin[p, xi + 1, body, :], ratio[xi])
            spin[p, xi + 1, body, :] = s
            energy = energy - fold(s * local[xi])
            own = own + fold(s * field[p, xi])
        wait_halo(p)
        if not final:
            gx_, gy_, gz_ = load_ghosts(p)
            nx_, ny_, nz_ = received(p, q)
            store_ghosts(p, after(gx_, nx_), (after(gy_[0], ny_[0]), after(gy_[1], ny_[1])), after(gz_, nz_))
            place_ghosts(p)
            send_rates(q, rates(q), energy)
            send_halo(q, lambda xi: ratio[xi], p)
        return own, energy, clock, table

    pl.semaphore_wait(barrier, count - 1)
    for p in range(2):
        send_halo(2 + p, lambda xi: spin[p, xi + 1, body, :], 1 - p)
    for load in loads[1:3]:
        load.wait()
    field_sum = lax.fori_loop(0, planes // 2, prepare_rest, zero)
    loads[3].wait()
    set_draws(0, 0)
    for p in (1, 0):
        wait_halo(2 + p)
        store_ghosts(p, *received(2 + p, 1 - p))
    place_ghosts(1)
    send_rates(0, rates(0), zero)
    send_halo(0, lambda xi: ratio[xi], 1)

    def pair(m, carry):
        carry = section(2 * m, 0, carry, False)
        return section(2 * m + 1, 1, carry, False)

    carry = (field_sum, zero, jnp.zeros((1, 1), jnp.float32), zero)
    carry = lax.fori_loop(0, SECTIONS // 2 - 1, pair, carry)
    carry = section(SECTIONS - 2, 0, carry, False)
    _, energy, _, table = section(SECTIONS - 1, 1, carry, True)
    send_rates(0, zero, energy)

    def finish(xi, none):
        flip = ((row + xi) & 1) == 1
        e, o = spin[0, xi + 1, body, :], spin[1, xi + 1, body, :]
        evens, odds = jnp.where(flip, o, e), jnp.where(flip, e, o)
        out[xi] = exact(jnp.where(low, evens, turn(odds, half)), join)
        out[xi + planes] = exact(jnp.where(low, turn(evens, half), odds), join)
        return none

    lax.fori_loop(0, planes, finish, 0)
    _, old = wait_rates(0)
    table = jnp.where((row8 == 0) & (lane8 == SECTIONS - 1), old / (2.0 * half_sites), table)
    hist[...] = table[0:2, 0:SECTIONS]


def hand_over(spins, table, out, hist):
    out[...] = spins[...]
    hist[...] = table[...]


def solution(mesh):
    sizes = tuple(mesh.shape[axis] for axis in AXES)

    def step(occupancy, site_field, attempt_rate, uniforms):
        nx, ny, nz = occupancy.shape
        planes = nx // 2
        tiles = ny // 8
        assert nx % 4 == 0 and ny % 8 == 0 and nz % 128 == 0 and planes * tiles <= nz // 2
        xdirs = 1 if sizes[0] == 2 else 2
        count = sizes[0] * sizes[1] * sizes[2]
        vmem = functools.partial(pl.BlockSpec, memory_space=pltpu.VMEM)
        f32 = jnp.float32
        made = pl.pallas_call(
            functools.partial(kernel, sizes),
            out_shape=(jax.ShapeDtypeStruct((nx, ny, nz), f32), jax.ShapeDtypeStruct((2, SECTIONS), f32)),
            in_specs=[pl.BlockSpec(memory_space=pl.ANY)] * 4,
            out_specs=(vmem(), vmem()),
            scratch_shapes=[
                pltpu.VMEM((nx, ny, nz), occupancy.dtype),
                pltpu.VMEM((nx, ny, nz), f32),
                pltpu.VMEM((nx, ny, nz), f32),
                pltpu.VMEM(uniforms.shape, f32),
                pltpu.SemaphoreType.DMA((4,)),
                pltpu.VMEM((2, planes + 2, ny + 2 * PAD, nz), f32),
                pltpu.VMEM((2, planes, ny, nz), f32),
                pltpu.VMEM((2, planes, ny, nz), f32),
                pltpu.VMEM((2, planes, ny, nz), f32),
                pltpu.VMEM((planes, ny, nz), f32),
                pltpu.VMEM((planes, ny, nz), f32),
                pltpu.VMEM((planes, ny, nz), f32),
                pltpu.VMEM((2, tiles + 3, 8, nz), f32),
                pltpu.VMEM((4, tiles + 3, 8, nz), f32),
                pltpu.VMEM((4, tiles * xdirs + 4, 8, nz), f32),
                pltpu.VMEM((2, 1, nz), f32),
                pltpu.VMEM((2, count, 1, nz), f32),
                pltpu.SemaphoreType.DMA((4,)),
                pltpu.SemaphoreType.DMA((4,)),
                pltpu.SemaphoreType.DMA((2,)),
                pltpu.SemaphoreType.DMA((2,)),
            ],
            compiler_params=pltpu.CompilerParams(collective_id=0, has_side_effects=True),
        )(occupancy, site_field, attempt_rate, uniforms)
        return pl.pallas_call(
            hand_over,
            out_shape=(jax.ShapeDtypeStruct((nx, ny, nz), f32), jax.ShapeDtypeStruct((2, SECTIONS), f32)),
            in_specs=[vmem()] * 2,
            out_specs=(vmem(), vmem()),
        )(*made)

    in_specs = (P("gx", "gy", "gz"), P("gx", "gy", "gz"), P("gx", "gy", "gz"), P(None, "gx", "gy", "gz"))
    return jax.shard_map(step, mesh=mesh, in_specs=in_specs, out_specs=(P("gx", "gy", "gz"), P()), check_vma=False)
```

```python
import functools
import itertools

import jax
import jax.numpy as jnp
from jax import lax
from jax.experimental import pallas as pl
from jax.experimental.pallas import tpu as pltpu
from jax.sharding import PartitionSpec as P

SECTIONS = 8
AXES = ("gx", "gy", "gz")
MESH = pl.DeviceIdType.MESH
PAD = 8


def kernel(sizes, occ_hbm, fld_hbm, att_hbm, uni_hbm, out, hist, occ, fld, att, uni, loaded, spin, field, rate0, inv, draw, ratio, local, ghost, hsend, hrecv,
           rsend, rrecv, hs, hr, rs, rr):
    gx, gy, gz = sizes
    count = gx * gy * gz
    planes, rows, lanes = ratio.shape
    half = lanes // 2
    tiles = rows // 8
    body = pl.ds(PAD, rows)
    xdirs = 1 if gx == 2 else 2
    ybase, zbase = tiles * xdirs, tiles * xdirs + 2
    loads = [pltpu.make_async_copy(a, b, loaded.at[i]) for i, (a, b) in enumerate(((occ_hbm, occ), (fld_hbm, fld), (att_hbm, att), (uni_hbm, uni)))]
    for load in loads:
        load.start()
    half_sites = float(planes * rows * lanes * count)
    pos = [lax.axis_index(axis) for axis in AXES]
    me = (pos[0] * gy + pos[1]) * gz + pos[2]
    moved = [[lax.rem(pos[a] + d, sizes[a]) for d in range(sizes[a])] for a in range(3)]

    def device(dx, dy, dz):
        return (moved[0][dx % gx], moved[1][dy % gy], moved[2][dz % gz])

    others = [o for o in itertools.product(range(gx), range(gy), range(gz)) if o != (0, 0, 0)]
    others.sort(key=lambda o: -(min(o[0], gx - o[0]) + min(o[1], gy - o[1]) + 4 * (o[2] % 2) + 2 * (o[2] > 0)))

    barrier = pltpu.get_barrier_semaphore()
    for o in others:
        pl.semaphore_signal(barrier, inc=1, device_id=device(*o), device_id_type=MESH)

    lane = lax.broadcasted_iota(jnp.int32, (rows, lanes), 1)
    row = lax.broadcasted_iota(jnp.int32, (rows, lanes), 0)
    low = lane < half
    place = lax.rem(lane, half)
    last = place == half - 1
    even = (row & 1) == 0
    odd = (row & 1) == 1
    lane8 = lax.broadcasted_iota(jnp.int32, (8, lanes), 1)
    row8 = lax.broadcasted_iota(jnp.int32, (8, lanes), 0)

    def kind(parity):
        return even if parity % 2 == 0 else odd

    def turn(x, shift):
        return pltpu.roll(x, shift % lanes, 1)

    zrow = lax.broadcasted_iota(jnp.int32, (lanes, lanes), 0)
    zcol = lax.broadcasted_iota(jnp.int32, (lanes, lanes), 1)
    split = (zrow == 2 * lax.rem(zcol, half) + zcol // half).astype(jnp.float32)
    join = (zcol == 2 * lax.rem(zrow, half) + zrow // half).astype(jnp.float32)

    def exact(a, b):
        return jnp.dot(a, b, precision=lax.Precision.HIGHEST, preferred_element_type=jnp.float32)

    split16 = split.astype(jnp.bfloat16)
    split48 = jnp.concatenate([split16] * 3, axis=0)

    def packed(ref, xi, n, whole):
        both = jnp.concatenate([ref[pl.ds(xi, n)].reshape(n * rows, lanes), ref[pl.ds(xi + planes, n)].reshape(n * rows, lanes)], axis=0)
        if whole:
            parts = both.astype(jnp.float32).astype(jnp.bfloat16)
        else:
            high = both.astype(jnp.bfloat16)
            rest = both - high.astype(jnp.float32)
            middle = rest.astype(jnp.bfloat16)
            parts = jnp.concatenate([high, middle, (rest - middle.astype(jnp.float32)).astype(jnp.bfloat16)], axis=1)
        moved = jnp.dot(parts, split16 if whole else split48, preferred_element_type=jnp.float32)
        for i in range(n):
            first, second = moved[i * rows:(i + 1) * rows], moved[(n + i) * rows:(n + i + 1) * rows]
            evens = jnp.where(low, first, turn(second, half))
            odds = jnp.where(low, turn(first, half), second)
            flip = ((row + xi + i) & 1) == 1
            yield xi + i, (jnp.where(flip, odds, evens), jnp.where(flip, evens, odds))

    def prepare_spins(group, none):
        for xi, s in packed(occ, 2 * group, 2, True):
            for p in range(2):
                spin[p, xi + 1, body, :] = 2.0 * s[p] - 1.0
        return none

    def prepare_rest(group, sums):
        for xi, f in packed(fld, 2 * group, 2, False):
            for p in range(2):
                field[p, xi] = f[p]
            sums = sums + fold(f[1] * spin[1, xi + 1, body, :])
        for xi, a in packed(att, 2 * group, 2, False):
            for p in range(2):
                rate0[p, xi] = a[p]
                inv[p, xi] = 1.0 / a[p]
        return sums

    def fold(x):
        return jnp.sum(x.reshape(tiles, 8, lanes), axis=0)

    zero = jnp.zeros((8, lanes), jnp.float32)
    loads[0].wait()
    lax.fori_loop(0, planes // 2, prepare_spins, 0)

    def set_draws(k, p):
        for xi in range(planes):
            both = jnp.concatenate([uni[k, xi], uni[k, xi + planes]], axis=1)
            draw[xi] = both * inv[p, xi]

    def halo_copy(slot, a, b, n, target):
        pltpu.make_async_remote_copy(hsend.at[slot, pl.ds(a, n)], hrecv.at[slot, pl.ds(b, n)], hs.at[slot], hr.at[slot],
                                     device_id=target, device_id_type=MESH).start()

    def send_halo(slot, plane, user):
        tail = jnp.zeros((rows, lanes), jnp.float32)
        for xi in range(planes):
            full = plane(xi)
            ends = jnp.where(kind(xi + user), full, turn(full, -1))
            tail = tail + jnp.where(place == half - 1 - xi, turn(ends, -xi), 0.0)
        z = tail[0:8]
        for t in range(1, tiles):
            z = z + turn(tail[8 * t:8 * t + 8], -planes * t)
        hsend[slot, tiles + 2] = z
        halo_copy(slot, tiles + 2, zbase, 1, device(0, 0, 1))
        halo_copy(slot, tiles + 2, zbase + 1, 1, device(0, 0, -1))
        hsend[slot, pl.ds(0, tiles)] = jnp.where(low, plane(0), plane(planes - 1)).reshape(tiles, 8, lanes)
        if xdirs == 1:
            halo_copy(slot, 0, 0, tiles, device(1, 0, 0))
        else:
            halo_copy(slot, 0, 0, tiles, device(-1, 0, 0))
            halo_copy(slot, 0, tiles, tiles, device(1, 0, 0))
        for xi in range(planes):
            full = plane(xi)
            hsend[slot, tiles, pl.ds(xi, 1), :] = full[0:1]
            hsend[slot, tiles + 1, pl.ds(xi, 1), :] = full[rows - 1:rows]
        halo_copy(slot, tiles, ybase, 1, device(0, -1, 0))
        halo_copy(slot, tiles + 1, ybase + 1, 1, device(0, 1, 0))

    def wait_halo(slot):
        whole = hrecv.at[slot]
        pltpu.make_async_copy(whole, whole, hr.at[slot]).wait()
        pltpu.make_async_copy(whole, whole, hs.at[slot]).wait()

    def received(slot, user):
        xs = hrecv[slot, pl.ds(0, tiles)].reshape(rows, lanes)
        if xdirs == 2:
            xs = jnp.where(low, xs, hrecv[slot, pl.ds(tiles, tiles)].reshape(rows, lanes))
        ys = (hrecv[slot, ybase], hrecv[slot, ybase + 1])
        down = ((lane8 + 1 + row8 + user) & 1) == 0
        return xs, ys, jnp.where(down, hrecv[slot, zbase], hrecv[slot, zbase + 1])

    def store_ghosts(p, xs, ys, zs):
        ghost[p, pl.ds(0, tiles)] = xs.reshape(tiles, 8, lanes)
        ghost[p, tiles], ghost[p, tiles + 1] = ys
        ghost[p, tiles + 2] = zs

    def load_ghosts(p):
        return ghost[p, pl.ds(0, tiles)].reshape(rows, lanes), (ghost[p, tiles], ghost[p, tiles + 1]), ghost[p, tiles + 2]

    def place_ghosts(p):
        xs, (above, below), _ = load_ghosts(p)
        spin[p, 0, body, :] = turn(jnp.where(low, spin[p, planes, body, :], xs), half)
        spin[p, planes + 1, body, :] = turn(jnp.where(low, xs, spin[p, 1, body, :]), half)
        for xi in range(planes):
            spin[p, xi + 1, pl.ds(PAD - 1, 1), :] = below[xi:xi + 1]
            spin[p, xi + 1, pl.ds(PAD + rows, 1), :] = above[xi:xi + 1]

    def rates(q):
        p = 1 - q
        zs = ghost[p, tiles + 2]
        ztile = jnp.concatenate([turn(zs, planes * t + half) for t in range(tiles)], axis=0)
        total = zero
        for xi in range(planes):
            mid = spin[p, xi + 1, body, :]
            edge = turn(ztile, xi)
            before = turn(jnp.where(last, edge, mid), 1)
            after = jnp.where(last, edge, turn(mid, -1))
            beside = spin[p, xi, body, :] + spin[p, xi + 2, body, :]
            beside = beside + spin[p, xi + 1, pl.ds(PAD - 1, rows), :] + spin[p, xi + 1, pl.ds(PAD + 1, rows), :]
            beside = beside + mid + jnp.where(kind(xi + q), before, after)
            h = field[q, xi] - 0.5 * beside
            grown = 1.0 + jnp.exp(2.0 * spin[q, xi + 1, body, :] * h)
            r = draw[xi] * grown
            ratio[xi] = r * r
            local[xi] = h
            total = total + fold(rate0[q, xi] / grown)
        return total

    def send_rates(slot, rate, energy):
        both = jnp.where(lane8 < half, rate + turn(rate, half), energy + turn(energy, half))
        message = jnp.sum(both, axis=0, keepdims=True)
        rsend[slot] = message
        rrecv[slot, me] = message
        for o in others:
            pltpu.make_async_remote_copy(rsend.at[slot], rrecv.at[slot, me], rs.at[slot], rr.at[slot],
                                         device_id=device(*o), device_id_type=MESH).start()

    def wait_rates(slot):
        most = rrecv.at[slot, pl.ds(0, count - 1)]
        pltpu.make_async_copy(most, most, rr.at[slot]).wait()
        pltpu.make_async_copy(most, most, rs.at[slot]).wait()
        total = jnp.sum(rrecv[slot], axis=0)
        first = lax.broadcasted_iota(jnp.int32, (1, lanes), 1) < half
        rate = jnp.sum(jnp.where(first, total, 0.0), axis=1, keepdims=True)
        energy = jnp.sum(jnp.where(first, 0.0, total), axis=1, keepdims=True)
        return rate, energy

    def section(k, p, carry, final):
        fields, energy, clock, table = carry
        q = 1 - p
        if not final:
            set_draws(k + 1, q)
        rate, old = wait_rates(p)
        table = jnp.where((row8 == 0) & (lane8 == k - 1), old / (2.0 * half_sites), table)
        clock = clock + half_sites / rate
        table = jnp.where((row8 == 1) & (lane8 == k), clock, table)
        scaled = rate * (1.0 / half_sites)
        c = scaled * scaled

        def after(s, x):
            xc = x * c
            return s * ((xc - 1.0) / (xc + 1.0))

        energy, own = -fields, zero
        for xi in range(planes):
            s = after(spin[p, xi + 1, body, :], ratio[xi])
            spin[p, xi + 1, body, :] = s
            energy = energy - fold(s * local[xi])
            own = own + fold(s * field[p, xi])
        wait_halo(p)
        if not final:
            gx_, gy_, gz_ = load_ghosts(p)
            nx_, ny_, nz_ = received(p, q)
            store_ghosts(p, after(gx_, nx_), (after(gy_[0], ny_[0]), after(gy_[1], ny_[1])), after(gz_, nz_))
            place_ghosts(p)
            send_rates(q, rates(q), energy)
            send_halo(q, lambda xi: ratio[xi], p)
        return own, energy, clock, table

    pl.semaphore_wait(barrier, count - 1)
    for p in (1, 0):
        send_halo(2 + p, lambda xi: spin[p, xi + 1, body, :], 1 - p)
    for load in loads[1:3]:
        load.wait()
    field_sum = lax.fori_loop(0, planes // 2, prepare_rest, zero)
    loads[3].wait()
    set_draws(0, 0)
    wait_halo(3)
    store_ghosts(1, *received(3, 0))
    place_ghosts(1)
    send_rates(0, rates(0), zero)
    send_halo(0, lambda xi: ratio[xi], 1)
    wait_halo(2)
    store_ghosts(0, *received(2, 1))

    def pair(m, carry):
        carry = section(2 * m, 0, carry, False)
        return section(2 * m + 1, 1, carry, False)

    carry = (field_sum, zero, jnp.zeros((1, 1), jnp.float32), zero)
    carry = lax.fori_loop(0, SECTIONS // 2 - 1, pair, carry)
    carry = section(SECTIONS - 2, 0, carry, False)
    _, energy, _, table = section(SECTIONS - 1, 1, carry, True)
    send_rates(0, zero, energy)

    def finish(xi, none):
        flip = ((row + xi) & 1) == 1
        e, o = spin[0, xi + 1, body, :], spin[1, xi + 1, body, :]
        evens, odds = jnp.where(flip, o, e), jnp.where(flip, e, o)
        fld[xi] = exact(jnp.where(low, evens, turn(odds, half)), join)
        fld[xi + planes] = exact(jnp.where(low, turn(evens, half), odds), join)
        return none

    lax.fori_loop(0, planes, finish, 0)
    store = pltpu.make_async_copy(fld, out, loaded.at[0])
    store.start()
    _, old = wait_rates(0)
    table = jnp.where((row8 == 0) & (lane8 == SECTIONS - 1), old / (2.0 * half_sites), table)
    hist[...] = table[0:2, 0:SECTIONS]
    store.wait()


def hand_over(spins, table, out, hist):
    out[...] = spins[...]
    hist[...] = table[...]


def solution(mesh):
    sizes = tuple(mesh.shape[axis] for axis in AXES)

    def step(occupancy, site_field, attempt_rate, uniforms):
        nx, ny, nz = occupancy.shape
        planes = nx // 2
        tiles = ny // 8
        assert nx % 4 == 0 and ny % 8 == 0 and nz % 128 == 0 and planes * tiles <= nz // 2
        xdirs = 1 if sizes[0] == 2 else 2
        count = sizes[0] * sizes[1] * sizes[2]
        vmem = functools.partial(pl.BlockSpec, memory_space=pltpu.VMEM)
        f32 = jnp.float32
        made = pl.pallas_call(
            functools.partial(kernel, sizes),
            out_shape=(jax.ShapeDtypeStruct((nx, ny, nz), f32), jax.ShapeDtypeStruct((2, SECTIONS), f32)),
            in_specs=[pl.BlockSpec(memory_space=pl.ANY)] * 4,
            out_specs=(pl.BlockSpec(memory_space=pl.ANY), vmem()),
            scratch_shapes=[
                pltpu.VMEM((nx, ny, nz), occupancy.dtype),
                pltpu.VMEM((nx, ny, nz), f32),
                pltpu.VMEM((nx, ny, nz), f32),
                pltpu.VMEM(uniforms.shape, f32),
                pltpu.SemaphoreType.DMA((4,)),
                pltpu.VMEM((2, planes + 2, ny + 2 * PAD, nz), f32),
                pltpu.VMEM((2, planes, ny, nz), f32),
                pltpu.VMEM((2, planes, ny, nz), f32),
                pltpu.VMEM((2, planes, ny, nz), f32),
                pltpu.VMEM((planes, ny, nz), f32),
                pltpu.VMEM((planes, ny, nz), f32),
                pltpu.VMEM((planes, ny, nz), f32),
                pltpu.VMEM((2, tiles + 3, 8, nz), f32),
                pltpu.VMEM((4, tiles + 3, 8, nz), f32),
                pltpu.VMEM((4, tiles * xdirs + 4, 8, nz), f32),
                pltpu.VMEM((2, 1, nz), f32),
                pltpu.VMEM((2, count, 1, nz), f32),
                pltpu.SemaphoreType.DMA((4,)),
                pltpu.SemaphoreType.DMA((4,)),
                pltpu.SemaphoreType.DMA((2,)),
                pltpu.SemaphoreType.DMA((2,)),
            ],
            compiler_params=pltpu.CompilerParams(collective_id=0, has_side_effects=True),
        )(occupancy, site_field, attempt_rate, uniforms)
        return pl.pallas_call(
            hand_over,
            out_shape=(jax.ShapeDtypeStruct((nx, ny, nz), f32), jax.ShapeDtypeStruct((2, SECTIONS), f32)),
            in_specs=[vmem()] * 2,
            out_specs=(vmem(), vmem()),
        )(*made)

    in_specs = (P("gx", "gy", "gz"), P("gx", "gy", "gz"), P("gx", "gy", "gz"), P(None, "gx", "gy", "gz"))
    return jax.shard_map(step, mesh=mesh, in_specs=in_specs, out_specs=(P("gx", "gy", "gz"), P()), check_vma=False)
```
